32 devices in a mesh: data: 1 (over z), pp: 4 (over y), ep: 8 (over x, core).
Axes of the slice: x: 4, y: 4, z: 1, core: 2. Of those that a mesh axis runs over, the one named last changes fastest.
The devices are a block of a 4x4x8 slice.
Arguments:
- expert_out: bfloat16 [4, 1, 64, 768, 2560], P(('data', 'pp'), None, 'ep')
- expert_ids: int32 [4, 1, 8, 512, 6], P(('data', 'pp'), None, 'ep')
- slot_ids: int32 [4, 1, 8, 512, 6], P(('data', 'pp'), None, 'ep')
- gates: float32 [4, 1, 8, 512, 6], P(('data', 'pp'), None, 'ep')
- resid: bfloat16 [4, 1, 8, 512, 2560], P(('data', 'pp'), None, 'ep')
- norm_scale: float32 [4, 2560], P('pp')
- w_query: bfloat16 [4, 2560, 2560], P('pp')
- w_key: bfloat16 [4, 2560, 2560], P('pp')
- w_value: bfloat16 [4, 2560, 2560], P('pp')
- w_out: bfloat16 [4, 20, 128, 2560], P('pp')
Outputs:
- output: bfloat16 [4, 1, 8, 512, 2560], P(('data', 'pp'), None, 'ep')
All inputs are finite; a program needn't handle non-finite values.
Results may differ from the reference program's by a relative error of at most 0.0119935.
Values are sent between devices in bfloat16 or wider.
A program may use at most 768 MiB of HBM per device.

```python
import jax
import jax.numpy as jnp
from jax import lax

STAGES = 4
EP_DEVS = 8
MICRO = 1
SEQ_DEV = 1
SEQ_LEN = 512
MODEL_DIM = 2560
EXPERTS = 64
TOP_K = 6
HEADS = 20
HEAD_DIM = 128

TOK_DEV = SEQ_DEV * SEQ_LEN
TOKENS = TOK_DEV * EP_DEVS
SEQ_COUNT = SEQ_DEV * EP_DEVS
SLOT_DEV = 2 * TOK_DEV * TOP_K // EXPERTS
CAPACITY = SLOT_DEV * EP_DEVS
HOT_EXPERTS = EXPERTS // 4
HOT_PICKS = TOP_K // 2
HIDDEN = HEADS * HEAD_DIM
NORM_EPS = 1e-6
TOKEN_SHAPE = (STAGES, MICRO, SEQ_COUNT, SEQ_LEN)


def rank_in_group(group_ids):
    count = group_ids.shape[0]
    order = jnp.argsort(group_ids * count + jnp.arange(count))
    sorted_ids = group_ids[order]
    first_pos = jnp.searchsorted(sorted_ids, sorted_ids, side='left')
    sorted_rank = (jnp.arange(count) - first_pos).astype(jnp.int32)
    return jnp.zeros((count,), jnp.int32).at[order].set(sorted_rank)


def draw_group(group_key):
    perm_key, hot_key, cold_key = jax.random.split(group_key, 3)
    expert_order = jax.random.permutation(perm_key, EXPERTS)
    hot_list = expert_order[:HOT_EXPERTS]
    cold_list = expert_order[HOT_EXPERTS:]
    hot_score = jax.random.randint(hot_key, (TOKENS, HOT_EXPERTS), 0, 65536) * HOT_EXPERTS + jnp.arange(HOT_EXPERTS)
    cold_score = jax.random.randint(cold_key, (TOKENS, EXPERTS - HOT_EXPERTS), 0, 65536) * EXPERTS + jnp.arange(EXPERTS - HOT_EXPERTS)
    hot_pick = jnp.argsort(hot_score, axis=1)[:, :HOT_PICKS]
    cold_pick = jnp.argsort(cold_score, axis=1)[:, :TOP_K - HOT_PICKS]
    chosen = jnp.concatenate([hot_list[hot_pick], cold_list[cold_pick]], axis=1).astype(jnp.int32)
    ranks = jax.vmap(rank_in_group)(chosen.reshape(EP_DEVS, TOK_DEV * TOP_K))
    slot_base = (jnp.arange(EP_DEVS, dtype=jnp.int32) * SLOT_DEV)[:, None]
    slots = jnp.where(ranks < SLOT_DEV, ranks + slot_base, -1).astype(jnp.int32)
    return chosen, slots.reshape(TOKENS, TOP_K)


def draw_routing(route_key):
    group_keys = jax.random.split(route_key, STAGES * MICRO)
    chosen, slots = lax.map(draw_group, group_keys)
    full_shape = TOKEN_SHAPE + (TOP_K,)
    return chosen.reshape(full_shape), slots.reshape(full_shape)


def draw_stage_out(stage_key):
    scale_key, value_key = jax.random.split(stage_key)
    expert_scale = jnp.exp(0.5 * jax.random.normal(scale_key, (MICRO, EXPERTS, 1, 1), jnp.float32))
    raw_out = jax.random.normal(value_key, (MICRO, EXPERTS, CAPACITY, MODEL_DIM), jnp.float32)
    return (raw_out * expert_scale).astype(jnp.bfloat16)


def setup_inputs(seed: int = 0, part: int = 0) -> dict:
    part_key = jax.random.fold_in(jax.random.key(seed), part)
    route_key, gate_key, resid_key, out_key = jax.random.split(part_key, 4)
    shared = jax.random.split(jax.random.key(seed + 1), 5)
    expert_ids, slot_ids = draw_routing(route_key)
    gate_logits = 1.5 * jax.random.normal(gate_key, TOKEN_SHAPE + (TOP_K,), jnp.float32)
    gates = 2.0 * jax.nn.softmax(gate_logits, axis=-1)
    resid = jax.random.normal(resid_key, TOKEN_SHAPE + (MODEL_DIM,), jnp.float32).astype(jnp.bfloat16)
    expert_out = lax.map(draw_stage_out, jax.random.split(out_key, STAGES))
    norm_scale = 1.0 + 0.5 * jax.random.normal(shared[0], (STAGES, MODEL_DIM), jnp.float32)
    in_scale = MODEL_DIM ** -0.5
    w_query = (1.5 * in_scale * jax.random.normal(shared[1], (STAGES, MODEL_DIM, HIDDEN), jnp.float32)).astype(jnp.bfloat16)
    w_key = (in_scale * jax.random.normal(shared[2], (STAGES, MODEL_DIM, HIDDEN), jnp.float32)).astype(jnp.bfloat16)
    w_value = (in_scale * jax.random.normal(shared[3], (STAGES, MODEL_DIM, HIDDEN), jnp.float32)).astype(jnp.bfloat16)
    w_out = (2.0 * HIDDEN ** -0.5 * jax.random.normal(shared[4], (STAGES, HEADS, HEAD_DIM, MODEL_DIM), jnp.float32)).astype(jnp.bfloat16)
    return {'expert_out': expert_out, 'expert_ids': expert_ids, 'slot_ids': slot_ids, 'gates': gates, 'resid': resid, 'norm_scale': norm_scale, 'w_query': w_query, 'w_key': w_key, 'w_value': w_value, 'w_out': w_out}


def combine_group(group_args):
    row_table, flat_ids, weights, resid_rows = group_args
    running = resid_rows.astype(jnp.float32)
    for choice in range(TOP_K):
        running = running + weights[:, choice, None] * row_table[flat_ids[:, choice]].astype(jnp.float32)
    return running.astype(jnp.bfloat16)


def attend_sequence(seq_rows, gain_row, w_query, w_key, w_value, w_out):
    x_float = seq_rows.astype(jnp.float32)
    inv_rms = lax.rsqrt(jnp.mean(x_float * x_float, axis=-1, keepdims=True) + NORM_EPS)
    normed = (x_float * inv_rms * gain_row).astype(jnp.bfloat16)
    q_heads = jnp.dot(normed, w_query, preferred_element_type=jnp.float32).astype(jnp.bfloat16).reshape(SEQ_LEN, HEADS, HEAD_DIM)
    k_heads = jnp.dot(normed, w_key, preferred_element_type=jnp.float32).astype(jnp.bfloat16).reshape(SEQ_LEN, HEADS, HEAD_DIM)
    v_heads = jnp.dot(normed, w_value, preferred_element_type=jnp.float32).astype(jnp.bfloat16).reshape(SEQ_LEN, HEADS, HEAD_DIM)
    scores = jnp.einsum('qhe,khe->hqk', q_heads.astype(jnp.float32), k_heads.astype(jnp.float32)) * HEAD_DIM ** -0.5
    positions = jnp.arange(SEQ_LEN)
    causal = positions[:, None] >= positions[None, :]
    attn_prob = jax.nn.softmax(jnp.where(causal, scores, -jnp.inf), axis=-1).astype(jnp.bfloat16)
    context = jnp.einsum('hqk,khe->qhe', attn_prob.astype(jnp.float32), v_heads.astype(jnp.float32)).astype(jnp.bfloat16)
    proj = jnp.einsum('qhe,hed->qd', context.astype(jnp.float32), w_out.astype(jnp.float32)).astype(jnp.bfloat16)
    return (x_float + proj.astype(jnp.float32)).astype(jnp.bfloat16)


def reference(expert_out, expert_ids, slot_ids, gates, resid, norm_scale, w_query, w_key, w_value, w_out):
    groups = STAGES * MICRO
    row_table = expert_out.reshape(groups, EXPERTS * CAPACITY, MODEL_DIM)
    is_kept = slot_ids >= 0
    flat_ids = (expert_ids * CAPACITY + jnp.where(is_kept, slot_ids, 0)).reshape(groups, TOKENS, TOP_K)
    weights = jnp.where(is_kept, gates, 0.0).reshape(groups, TOKENS, TOP_K)
    resid_rows = resid.reshape(groups, TOKENS, MODEL_DIM)
    combined = lax.map(combine_group, (row_table, flat_ids, weights, resid_rows))
    shifted = jnp.roll(combined.reshape(STAGES, MICRO * SEQ_COUNT, SEQ_LEN, MODEL_DIM), 1, axis=0)

    def stage_block(stage_args):
        stage_seqs, gain_row, stage_query, stage_key, stage_value, stage_out = stage_args

        def one_sequence(seq_rows):
            return attend_sequence(seq_rows, gain_row, stage_query, stage_key, stage_value, stage_out)

        return lax.map(one_sequence, stage_seqs)

    result = lax.map(stage_block, (shifted, norm_scale, w_query, w_key, w_value, w_out))
    return result.reshape(TOKEN_SHAPE + (MODEL_DIM,))
```

```python
import functools

import jax
import jax.numpy as jnp
from jax import lax
from jax.experimental import pallas as pl
from jax.experimental.pallas import tpu as pltpu
from jax.sharding import PartitionSpec as P

NORM_EPS = 1e-6
CORES = 2
CHUNK = 128
MESH = pl.DeviceIdType.MESH
F32 = jnp.float32
BF16 = jnp.bfloat16


def combine_kernel(dims, meta_ref, eo_ref, h_ref, out_ref, obuf, metas, mt, wbuf, part, own, recv, ybuf,
                   o_loc, o_send, o_recv, m_send, m_recv, r_send, r_recv, y_send, y_recv):
    ring, stages, experts, slot_dev, width, seq_len, top_k = dims
    half = width // 2
    depth = CORES * experts * slot_dev
    chunks = seq_len // CHUNK
    col_tile = 256
    tiles = half // col_tile
    ep = lax.axis_index('ep')
    stage = lax.axis_index('pp')
    chip = ep // CORES
    core = ep % CORES
    other = 1 - core

    def chip_at(offset):
        return lax.rem(chip + offset + ring, ring)

    def ep_at(offset):
        return {'ep': chip_at(offset) * CORES + core}

    partner = {'ep': chip * CORES + other}
    next_stage = {'pp': lax.rem(stage + 1, stages)}
    prev_stage = {'pp': lax.rem(stage + stages - 1, stages)}
    offsets = (-1, 1, 2, 0)

    barrier = pltpu.get_barrier_semaphore()
    peers = (partner, ep_at(-1), ep_at(1), ep_at(2), next_stage, prev_stage)
    for peer in peers:
        pl.semaphore_signal(barrier, inc=1, device_id=peer, device_id_type=MESH)
    pl.semaphore_wait(barrier, len(peers))

    def own_rows(slot, side):
        rows = pl.ds((chip_at(offsets[slot]) * CORES + core) * slot_dev, slot_dev)
        return pltpu.make_async_copy(eo_ref.at[:, rows, pl.ds(side * half, half)], obuf.at[slot, side, core],
                                     o_loc.at[slot, side])

    def partner_rows(slot, side):
        rows = pl.ds((chip_at(offsets[slot]) * CORES + other) * slot_dev, slot_dev)
        return pltpu.make_async_remote_copy(
            src_ref=eo_ref.at[:, rows, pl.ds(side * half, half)], dst_ref=obuf.at[slot, side, core],
            send_sem=o_send.at[slot, side], recv_sem=o_recv.at[slot, side], device_id=partner, device_id_type=MESH)

    meta_copies = [pltpu.make_async_remote_copy(
        src_ref=meta_ref, dst_ref=metas.at[slot], send_sem=m_send.at[slot], recv_sem=m_recv.at[slot],
        device_id=ep_at(-offsets[slot]), device_id_type=MESH) for slot in range(3)]
    for copy in meta_copies:
        copy.start()
    order = ((0, 0), (1, 1), (0, 1), (1, 0), (2, 0), (2, 1), (3, 0), (3, 1))
    for slot, side in order:
        partner_rows(slot, side).start()
        own_rows(slot, side).start()

    ready = set()

    def need_rows(slot, side):
        if (slot, side) not in ready:
            ready.add((slot, side))
            own_rows(slot, side).wait()
            partner_rows(slot, side).wait_recv()

    def need_meta(slot):
        if slot < 3 and slot not in ready:
            ready.add(slot)
            meta_copies[slot].wait_recv()

    base = (chip * depth).astype(F32)
    lane = lax.broadcasted_iota(jnp.int32, (16, 128), 1).astype(F32) + base

    def build(bank, slot, q):
        need_meta(slot)
        cols = slice(q * CHUNK, (q + 1) * CHUNK)
        block = meta_ref[:, cols] if slot == 3 else metas[slot, :, cols]
        mt[...] = jnp.transpose(block)

        def rows_step(step, carry):
            at = pl.multiple_of(step * 16, 16)
            rows = mt[pl.ds(at, 16), :]
            keys = [jnp.broadcast_to(rows[:, k:k + 1], (16, 128)) for k in range(top_k)]
            gates = [jnp.broadcast_to(rows[:, 8 + k:9 + k], (16, 128)) for k in range(top_k)]
            for tile in range(depth // 128):
                place = lane + float(tile * 128)
                weight = jnp.zeros((16, 128), F32)
                for k in range(top_k):
                    weight = jnp.where(keys[k] == place, gates[k], weight)
                high = weight.astype(BF16)
                rest = weight - high.astype(F32)
                mid = rest.astype(BF16)
                low = (rest - mid.astype(F32)).astype(BF16)
                at_col = slice(tile * 128, (tile + 1) * 128)
                wbuf[bank, pl.ds(at, 16), at_col] = high
                wbuf[bank, pl.ds(CHUNK + at, 16), at_col] = mid
                wbuf[bank, pl.ds(2 * CHUNK + at, 16), at_col] = low
            return carry

        lax.fori_loop(0, CHUNK // 16, rows_step, 0)

    def product(bank, slot, side, tile):
        at = pl.multiple_of(tile * col_tile, col_tile)
        rows = obuf[slot, side, :, :, :, pl.ds(at, col_tile)].reshape(depth, col_tile)
        res = jnp.dot(wbuf[bank], rows, preferred_element_type=F32)
        return at, (res[2 * CHUNK:] + res[CHUNK:2 * CHUNK]) + res[:CHUNK]

    def weigh(bank, slot, side, dst):
        need_rows(slot, side)

        def step(tile, carry):
            at, value = product(bank, slot, side, tile)
            dst[:, pl.ds(at, col_tile)] = value
            return carry

        lax.fori_loop(0, tiles, step, 0)

    def ring_copy(q, step, way):
        src = part.at[q % 2, way, way] if step == 0 else recv.at[q, step - 1, way]
        return pltpu.make_async_remote_copy(
            src_ref=src, dst_ref=recv.at[q, step, way], send_sem=r_send.at[q, step, way], recv_sem=r_recv.at[q, step, way],
            device_id=ep_at(1 if way == 0 else -1), device_id_type=MESH)

    def add_part(q, step, way, slot):
        def rows_step(i, carry):
            at = pl.ds(pl.multiple_of(i * 16, 16), 16)
            recv[q, step, way, at, :] = recv[q, step, way, at, :] + part[q % 2, slot, way, at, :]
            return carry

        lax.fori_loop(0, CHUNK // 16, rows_step, 0)

    def stage_a(q):
        par = q % 2
        if q >= 2:
            for way in (0, 1):
                ring_copy(q - 2, 0, way).wait_send()
        build(0, 0, q)
        weigh(0, 0, 0, part.at[par, 0, 0])
        ring_copy(q, 0, 0).start()
        build(1, 1, q)
        weigh(1, 1, 1, part.at[par, 1, 1])
        ring_copy(q, 0, 1).start()
        weigh(0, 0, 1, part.at[par, 0, 1])
        weigh(1, 1, 0, part.at[par, 1, 0])

    def stage_b(q):
        build(0, 2, q)
        for way in (0, 1):
            weigh(0, 2, way, part.at[q % 2, 2, way])
        for way in (0, 1):
            ring_copy(q, 0, way).wait_recv()
            add_part(q, 0, way, 2)
            ring_copy(q, 1, way).start()

    def stage_c(q):
        for way in (0, 1):
            ring_copy(q, 1, way).wait_recv()
            add_part(q, 1, way, 1 - way)
            ring_copy(q, 2, way).start()

    def y_copy(q):
        rows = pl.ds(q * CHUNK, CHUNK)
        return pltpu.make_async_remote_copy(
            src_ref=ybuf.at[q], dst_ref=out_ref.at[rows, :], send_sem=y_send.at[q], recv_sem=y_recv.at[q],
            device_id=next_stage, device_id_type=MESH)

    def stage_d(q):
        build(0, 3, q)
        for way in (0, 1):
            weigh(0, 3, way, own.at[way])
        for way in (0, 1):
            ring_copy(q, 2, way).wait_recv()

            def rows_step(i, carry, way=way):
                at = pl.multiple_of(i * 16, 16)
                total = h_ref[pl.ds(q * CHUNK + at, 16), way * half:(way + 1) * half].astype(F32)
                total = total + (recv[q, 2, way, pl.ds(at, 16), :] + own[way, pl.ds(at, 16), :])
                ybuf[q, pl.ds(at, 16), way * half:(way + 1) * half] = total.astype(BF16)
                return carry

            lax.fori_loop(0, CHUNK // 16, rows_step, 0)
        y_copy(q).start()

    for first in range(0, chunks, 2):
        if first == 0:
            stage_a(0)
            stage_a(1)
        stage_b(first)
        stage_b(first + 1)
        stage_c(first)
        if first + 2 < chunks:
            stage_a(first + 2)
        stage_c(first + 1)
        if first + 3 < chunks:
            stage_a(first + 3)
        stage_d(first)
        stage_d(first + 1)

    for copy in meta_copies:
        copy.wait_send()
    for slot, side in order:
        partner_rows(slot, side).wait_send()
    for q in range(chunks):
        for way in (0, 1):
            for step in range(3):
                if step > 0 or q >= chunks - 2:
                    ring_copy(q, step, way).wait_send()
        y_copy(q).wait()


def combine_call(meta, expert_out, resid, ring, stages):
    experts, capacity, width = expert_out.shape
    seq_len = resid.shape[0]
    slot_dev = capacity // (ring * CORES)
    half = width // 2
    depth = CORES * experts * slot_dev
    chunks = seq_len // CHUNK
    top_k = 6
    dims = (ring, stages, experts, slot_dev, width, seq_len, top_k)
    dma = pltpu.SemaphoreType.DMA
    return pl.pallas_call(
        functools.partial(combine_kernel, dims),
        out_shape=jax.ShapeDtypeStruct((seq_len, width), BF16),
        in_specs=[pl.BlockSpec(memory_space=pltpu.VMEM), pl.BlockSpec(memory_space=pl.ANY),
                  pl.BlockSpec(memory_space=pltpu.VMEM)],
        out_specs=pl.BlockSpec(memory_space=pl.ANY),
        scratch_shapes=[
            pltpu.VMEM((4, 2, CORES, experts, slot_dev, half), BF16),
            pltpu.VMEM((3, 16, seq_len), F32),
            pltpu.VMEM((CHUNK, 16), F32),
            pltpu.VMEM((2, 3 * CHUNK, depth), BF16),
            pltpu.VMEM((2, 3, 2, CHUNK, half), F32),
            pltpu.VMEM((2, CHUNK, half), F32),
            pltpu.VMEM((chunks, 3, 2, CHUNK, half), F32),
            pltpu.VMEM((chunks, CHUNK, width), BF16),
            dma((4, 2)), dma((4, 2)), dma((4, 2)),
            dma((3,)), dma((3,)),
            dma((chunks, 3, 2)), dma((chunks, 3, 2)),
            dma((chunks,)), dma((chunks,)),
        ],
        compiler_params=pltpu.CompilerParams(collective_id=0, has_side_effects=True, vmem_limit_bytes=67_000_000),
        name='combine',
    )(meta, expert_out, resid)


def attend_kernel(head_dim, y_ref, gain_ref, wq_ref, wk_ref, wv_ref, wo_ref, z_ref, x_ref, acc_ref, ctx_ref):
    step = pl.program_id(0)
    last = pl.num_programs(0) - 1
    seq_len, width = y_ref.shape
    group = wq_ref.shape[1]
    block = 128

    @pl.when(step == 0)
    def _():
        def rows_step(i, carry):
            at = pl.ds(pl.multiple_of(i * 16, 16), 16)
            x = y_ref[at, :].astype(F32)
            inv_rms = lax.rsqrt(jnp.mean(x * x, axis=-1, keepdims=True) + NORM_EPS)
            x_ref[at, :] = (x * inv_rms * gain_ref[...]).astype(BF16)
            return carry

        lax.fori_loop(0, seq_len // 16, rows_step, 0)

    x = x_ref[...]
    q = jnp.dot(x, wq_ref[...], preferred_element_type=F32).astype(BF16)
    k = jnp.dot(x, wk_ref[...], preferred_element_type=F32).astype(BF16)
    v = jnp.dot(x, wv_ref[...], preferred_element_type=F32).astype(BF16)
    row = lax.broadcasted_iota(jnp.int32, (block, block), 0)
    col = lax.broadcasted_iota(jnp.int32, (block, block), 1)
    keep = row >= col
    for head in range(group // head_dim):
        lanes = slice(head * head_dim, (head + 1) * head_dim)
        for qb in range(seq_len // block):
            rows = slice(qb * block, (qb + 1) * block)
            seen = (qb + 1) * block
            s = lax.dot_general(q[rows, lanes], k[:seen, lanes], (((1,), (1,)), ((), ())),
                                preferred_element_type=F32) * head_dim ** -0.5
            diag = jnp.where(keep, s[:, qb * block:], -jnp.inf)
            s = diag if qb == 0 else jnp.concatenate([s[:, :qb * block], diag], axis=1)
            e = jnp.exp(s - jnp.max(s, axis=-1, keepdims=True))
            p = (e / jnp.sum(e, axis=-1, keepdims=True)).astype(BF16)
            ctx_ref[rows, lanes] = jnp.dot(p, v[:seen, lanes], preferred_element_type=F32).astype(BF16)

    ctx = ctx_ref[...]
    tile = 512

    @pl.when(step == 0)
    def _():
        for n in range(width // tile):
            cols = slice(n * tile, (n + 1) * tile)
            acc_ref[:, cols] = jnp.dot(ctx, wo_ref[:, cols], preferred_element_type=F32)

    @pl.when(step > 0)
    def _():
        for n in range(width // tile):
            cols = slice(n * tile, (n + 1) * tile)
            acc_ref[:, cols] += jnp.dot(ctx, wo_ref[:, cols], preferred_element_type=F32)

    @pl.when(step == last)
    def _():
        def rows_step(i, carry):
            at = pl.ds(pl.multiple_of(i * 16, 16), 16)
            proj = acc_ref[at, :].astype(BF16).astype(F32)
            z_ref[at, :] = (y_ref[at, :].astype(F32) + proj).astype(BF16)
            return carry

        lax.fori_loop(0, seq_len // 16, rows_step, 0)


def attend_call(arrived, gain, w_query, w_key, w_value, w_out, head_dim):
    seq_len, width = arrived.shape
    hidden = w_query.shape[1]
    group = 2 * head_dim
    whole = lambda i: (0, 0)
    in_col = pl.BlockSpec((width, group), lambda i: (0, i))
    return pl.pallas_call(
        functools.partial(attend_kernel, head_dim),
        grid=(hidden // group,),
        out_shape=jax.ShapeDtypeStruct((seq_len, width), BF16),
        in_specs=[pl.BlockSpec((seq_len, width), whole), pl.BlockSpec((1, width), whole), in_col, in_col, in_col,
                  pl.BlockSpec((group, width), lambda i: (i, 0))],
        out_specs=pl.BlockSpec((seq_len, width), whole),
        scratch_shapes=[pltpu.VMEM((seq_len, width), BF16), pltpu.VMEM((seq_len, width), F32),
                        pltpu.VMEM((seq_len, group), BF16)],
        compiler_params=pltpu.CompilerParams(vmem_limit_bytes=60_000_000),
        name='attend',
    )(arrived, gain, w_query, w_key, w_value, w_out)


def solution(mesh):
    stages = mesh.shape['pp']
    ep_size = mesh.shape['ep']
    ring = ep_size // CORES
    assert ring == 4
    token_spec = P(('data', 'pp'), None, 'ep', None, None)
    weight_spec = P('pp', None, None)

    def local_step(expert_out, expert_ids, slot_ids, gates, resid, norm_scale, w_query, w_key, w_value, w_out):
        experts, capacity, width = expert_out.shape[2:]
        slot_dev = capacity // ep_size
        ids, slots, gate = expert_ids[0, 0, 0], slot_ids[0, 0, 0], gates[0, 0, 0]
        keys = jnp.where(slots >= 0, ids * slot_dev + slots - lax.axis_index('ep') * slot_dev, -1).astype(F32)
        pad = ((0, 8 - keys.shape[1]), (0, 0))
        meta = jnp.concatenate([jnp.pad(keys.T, pad), jnp.pad(gate.T, pad)], axis=0)
        arrived = combine_call(meta, expert_out[0, 0], resid[0, 0, 0], ring, stages)
        heads, head_dim = w_out.shape[1:3]
        z = attend_call(arrived, norm_scale, w_query[0], w_key[0], w_value[0],
                        w_out[0].reshape(heads * head_dim, width), head_dim)
        return z[None, None, None]

    return jax.shard_map(local_step, mesh=mesh, in_specs=(token_spec, token_spec, token_spec, token_spec, token_spec, P('pp', None), weight_spec, weight_spec, weight_spec, P('pp', None, None, None)), out_specs=token_spec, check_vma=False)
```

```python
import functools

import jax
import jax.numpy as jnp
from jax import lax
from jax.experimental import pallas as pl
from jax.experimental.pallas import tpu as pltpu
from jax.sharding import PartitionSpec as P

NORM_EPS = 1e-6
CORES = 2
SIZES = (160, 144, 128, 80)
MESH = pl.DeviceIdType.MESH
F32 = jnp.float32
BF16 = jnp.bfloat16
LANES = 128
COLS = 256
DEEP = 3


def fused_kernel(dims, meta_ref, gain_ref, eo_ref, h_ref, wq_ref, wk_ref, wv_ref, wo_ref, z_ref, prow,
                 obuf, metas, mt, wbuf, part, recv, ybuf, yrecv, hbuf, wtile, kc, vc, xs, ctx, zbuf,
                 b_sem, o_send, o_recv, m_send, m_recv, r_send, r_recv, y_send, y_recv, h_sem, w_sem, z_sem):
    ring, stages, experts, slot_dev, width, seq_len, top_k, head_dim = dims
    half = width // 2
    depth = CORES * experts * slot_dev
    starts = [sum(SIZES[:q]) for q in range(len(SIZES))]
    chunks = len(SIZES)
    ep = lax.axis_index('ep')
    stage = lax.axis_index('pp')
    chip = ep // CORES
    core = ep % CORES
    other = 1 - core

    def chip_at(offset):
        return lax.rem(chip + offset + ring, ring)

    def ep_at(offset):
        return {'ep': chip_at(offset) * CORES + core}

    partner = {'ep': chip * CORES + other}
    next_stage = {'pp': lax.rem(stage + 1, stages)}
    prev_stage = {'pp': lax.rem(stage + stages - 1, stages)}
    offsets = (-1, 1, 2, 0)

    barrier = pltpu.get_barrier_semaphore()
    peers = (partner, ep_at(-1), ep_at(1), ep_at(2), next_stage, prev_stage)
    for peer in peers:
        pl.semaphore_signal(barrier, inc=1, device_id=peer, device_id_type=MESH)
    pl.semaphore_wait(barrier, len(peers))

    def partner_rows(slot, side):
        rows = pl.ds((chip_at(offsets[slot]) * CORES + other) * slot_dev, slot_dev)
        return pltpu.make_async_remote_copy(
            src_ref=eo_ref.at[:, rows, pl.ds(side * half, half)], dst_ref=prow.at[slot, side],
            send_sem=o_send.at[slot, side], recv_sem=o_recv.at[slot, side], device_id=partner, device_id_type=MESH)

    meta_copies = [pltpu.make_async_remote_copy(
        src_ref=meta_ref, dst_ref=metas.at[slot], send_sem=m_send.at[slot], recv_sem=m_recv.at[slot],
        device_id=ep_at(-offsets[slot]), device_id_type=MESH) for slot in range(3)]
    first_blocks = ((2, 0), (2, 1), (1, 1), (0, 0), (1, 0), (0, 1))
    own_blocks = ((3, 0), (3, 1))
    for copy in meta_copies:
        copy.start()
    for slot, side in first_blocks + own_blocks:
        partner_rows(slot, side).start()

    uses = list(first_blocks) + list(own_blocks) + list(first_blocks) * 2 + list(own_blocks) + list(first_blocks) \
        + list(own_blocks) * 2
    arrived = set()

    def block_copies(index):
        slot, side = uses[index]
        buf = index % 2
        rows = pl.ds((chip_at(offsets[slot]) * CORES + core) * slot_dev, slot_dev)
        mine = pltpu.make_async_copy(eo_ref.at[:, rows, pl.ds(side * half, half)], obuf.at[buf, core], b_sem.at[buf, 0])
        theirs = pltpu.make_async_copy(prow.at[slot, side], obuf.at[buf, other], b_sem.at[buf, 1])
        return mine, theirs

    def fetch_block(index):
        if index < len(uses):
            mine, theirs = block_copies(index)
            mine.start()
            if uses[index] not in arrived:
                arrived.add(uses[index])
                partner_rows(*uses[index]).wait_recv()
            theirs.start()

    pairs = width // COLS
    outs = pairs // 2
    steps = pairs + outs

    def qkv_copies(step, buf):
        cols = pl.ds(pl.multiple_of(step * COLS, COLS), COLS)
        return [pltpu.make_async_copy(ref.at[:, cols], wtile.at[buf, i], w_sem.at[buf, i])
                for i, ref in enumerate((wq_ref, wk_ref, wv_ref))]

    def out_copies(step, buf):
        return [pltpu.make_async_copy(wo_ref.at[:, pl.ds(pl.multiple_of(step * 2 * COLS + i * COLS, COLS), COLS)],
                                      wtile.at[buf, i], w_sem.at[buf, i]) for i in range(2)]

    def start_all(copies):
        for copy in copies:
            copy.start()

    fetch_block(0)
    for step in range(DEEP - 1):
        start_all(qkv_copies(step, step))

    def zero_step(i, carry):
        at = pl.ds(pl.multiple_of(i * 16, 16), 16)
        kc[at, :] = jnp.zeros((16, width), BF16)
        vc[at, :] = jnp.zeros((16, width), BF16)
        return carry

    lax.fori_loop(0, seq_len // 16, zero_step, 0)

    base = (chip * depth).astype(F32)
    lane = lax.broadcasted_iota(jnp.int32, (16, LANES), 1).astype(F32) + base
    met = set()

    def build(bank, slot, q):
        if slot < 3 and slot not in met:
            met.add(slot)
            meta_copies[slot].wait_recv()
        size = SIZES[q]
        for lo in range(0, seq_len, LANES):
            if lo < starts[q] + size and lo + LANES > starts[q]:
                cols = slice(lo, lo + LANES)
                block = meta_ref[:, cols] if slot == 3 else metas[slot, :, cols]
                mt[lo:lo + LANES, :] = jnp.transpose(block)

        def rows_step(step, carry):
            at = pl.multiple_of(step * 16, 16)
            rows = mt[pl.ds(starts[q] + at, 16), :]
            keys = [jnp.broadcast_to(rows[:, k:k + 1], (16, LANES)) for k in range(top_k)]
            gates = [jnp.broadcast_to(rows[:, 8 + k:9 + k], (16, LANES)) for k in range(top_k)]
            for tile in range(depth // LANES):
                place = lane + float(tile * LANES)
                weight = jnp.zeros((16, LANES), F32)
                for k in range(top_k):
                    weight = jnp.where(keys[k] == place, gates[k], weight)
                high = weight.astype(BF16)
                rest = weight - high.astype(F32)
                mid = rest.astype(BF16)
                low = (rest - mid.astype(F32)).astype(BF16)
                at_col = slice(tile * LANES, (tile + 1) * LANES)
                wbuf[bank, pl.ds(at, 16), at_col] = high
                wbuf[bank, pl.ds(size + at, 16), at_col] = mid
                wbuf[bank, pl.ds(2 * size + at, 16), at_col] = low
            return carry

        lax.fori_loop(0, size // 16, rows_step, 0)

    used = [0]

    def weigh(bank, slot, side, q, dst):
        index = used[0]
        used[0] += 1
        assert uses[index] == (slot, side)
        size = SIZES[q]
        buf = index % 2
        fetch_block(index + 1)
        for copy in block_copies(index):
            copy.wait()

        def step(tile, carry):
            at = pl.multiple_of(tile * COLS, COLS)
            rows = obuf[buf, :, :, :, pl.ds(at, COLS)].reshape(depth, COLS)
            res = jnp.dot(wbuf[bank, :3 * size], rows, preferred_element_type=F32)
            dst[:size, pl.ds(at, COLS)] = (res[2 * size:] + res[size:2 * size]) + res[:size]
            return carry

        lax.fori_loop(0, half // COLS, step, 0)

    sent = (((2, 0), (2, 1)), ((1, 1), (0, 0)), ((1, 0), (0, 1)))

    def ring_copy(q, kind, way):
        slot, side = sent[kind][way]
        rows = pl.ds(starts[q], SIZES[q])
        return pltpu.make_async_remote_copy(
            src_ref=part.at[q % 2, slot, side, pl.ds(0, SIZES[q])], dst_ref=recv.at[kind, way, rows],
            send_sem=r_send.at[q, kind, way], recv_sem=r_recv.at[q, kind, way],
            device_id=ep_at(1 if way == 0 else -1), device_id_type=MESH)

    def residual(q):
        return pltpu.make_async_copy(h_ref.at[pl.ds(starts[q], SIZES[q])], hbuf.at[pl.ds(0, SIZES[q])], h_sem)

    def partials(q):
        par = part.at[q % 2]
        if q >= 2:
            for way in (0, 1):
                ring_copy(q - 2, 1, way).wait_send()
                ring_copy(q - 2, 2, way).wait_send()
        build(0, 2, q)
        weigh(0, 2, 0, q, par.at[2, 0])
        ring_copy(q, 0, 0).start()
        weigh(0, 2, 1, q, par.at[2, 1])
        ring_copy(q, 0, 1).start()
        build(1, 1, q)
        weigh(1, 1, 1, q, par.at[1, 1])
        ring_copy(q, 1, 0).start()
        build(0, 0, q)
        weigh(0, 0, 0, q, par.at[0, 0])
        ring_copy(q, 1, 1).start()
        weigh(1, 1, 0, q, par.at[1, 0])
        weigh(0, 0, 1, q, par.at[0, 1])

    def pass_on(q):
        for way in (0, 1):
            slot, side = sent[2][way]
            ring_copy(q, 0, way).wait_recv()

            def rows_step(i, carry, way=way, slot=slot, side=side):
                at = pl.multiple_of(i * 16, 16)
                mine = part[q % 2, slot, side, pl.ds(at, 16), :]
                part[q % 2, slot, side, pl.ds(at, 16), :] = mine + recv[0, way, pl.ds(starts[q] + at, 16), :]
                return carry

            lax.fori_loop(0, SIZES[q] // 16, rows_step, 0)
            ring_copy(q, 2, way).start()

    def own_partials(q):
        for way in (0, 1):
            ring_copy(q, 0, way).wait_send()
        build(0, 3, q)
        for side in (0, 1):
            weigh(0, 3, side, q, part.at[q % 2, 2, side])

    def y_copy(q):
        return pltpu.make_async_remote_copy(
            src_ref=ybuf.at[pl.ds(starts[q], SIZES[q])], dst_ref=yrecv.at[pl.ds(starts[q], SIZES[q])],
            send_sem=y_send.at[q], recv_sem=y_recv.at[q], device_id=next_stage, device_id_type=MESH)

    def finish(q):
        residual(q).wait()
        for way in (0, 1):
            ring_copy(q, 1, way).wait_recv()
            ring_copy(q, 2, way).wait_recv()
        for side in (0, 1):

            def rows_step(i, carry, side=side):
                at = pl.multiple_of(i * 16, 16)
                rows = pl.ds(starts[q] + at, 16)
                cols = slice(side * half, (side + 1) * half)
                total = part[q % 2, 2, side, pl.ds(at, 16), :]
                total = total + recv[1, 1 - side, rows, :]
                total = total + recv[2, side, rows, :]
                total = total + hbuf[pl.ds(at, 16), cols].astype(F32)
                ybuf[rows, cols] = total.astype(BF16)
                return carry

            lax.fori_loop(0, SIZES[q] // 16, rows_step, 0)
        y_copy(q).start()
        if q + 1 < chunks:
            residual(q + 1).start()

    def z_copy(q):
        return pltpu.make_async_copy(zbuf.at[pl.ds(0, SIZES[q])], z_ref.at[pl.ds(starts[q], SIZES[q])], z_sem)

    def attend(q, between=None):
        size, start = SIZES[q], starts[q]
        seen = -(-(start + size) // LANES) * LANES
        y_copy(q).wait_recv()

        def norm_step(i, carry):
            at = pl.multiple_of(i * 16, 16)
            x = yrecv[pl.ds(start + at, 16), :].astype(F32)
            inv_rms = lax.rsqrt(jnp.mean(x * x, axis=-1, keepdims=True) + NORM_EPS)
            xs[pl.ds(at, 16), :] = (x * inv_rms * gain_ref[...]).astype(BF16)
            return carry

        lax.fori_loop(0, size // 16, norm_step, 0)
        row = lax.broadcasted_iota(jnp.int32, (size, seen), 0) + start
        col = lax.broadcasted_iota(jnp.int32, (size, seen), 1)

        def head_step(step, carry):
            buf = lax.rem(step, DEEP)
            ahead = lax.rem(step + DEEP - 1, DEEP)

            @pl.when(step + DEEP - 1 < pairs)
            def _():
                start_all(qkv_copies(step + DEEP - 1, ahead))

            @pl.when(step + DEEP - 1 >= pairs)
            def _():
                start_all(out_copies(step + DEEP - 1 - pairs, ahead))

            for copy in qkv_copies(step, buf):
                copy.wait()
            x = xs[:size]
            lanes = pl.ds(pl.multiple_of(step * COLS, COLS), COLS)
            qh = jnp.dot(x, wtile[buf, 0], preferred_element_type=F32).astype(BF16)
            kc[pl.ds(start, size), lanes] = jnp.dot(x, wtile[buf, 1], preferred_element_type=F32).astype(BF16)
            vc[pl.ds(start, size), lanes] = jnp.dot(x, wtile[buf, 2], preferred_element_type=F32).astype(BF16)
            for head in range(COLS // head_dim):
                one = pl.ds(pl.multiple_of(step * COLS + head * head_dim, head_dim), head_dim)
                s = lax.dot_general(qh[:, head * head_dim:(head + 1) * head_dim], kc[:seen, one],
                                    (((1,), (1,)), ((), ())), preferred_element_type=F32) * head_dim ** -0.5
                s = jnp.where(row >= col, s, -jnp.inf)
                e = jnp.exp(s - jnp.max(s, axis=-1, keepdims=True))
                p = (e * (1.0 / jnp.sum(e, axis=-1, keepdims=True))).astype(BF16)
                ctx[:size, one] = jnp.dot(p, vc[:seen, one], preferred_element_type=F32).astype(BF16)
            return carry

        lax.fori_loop(0, pairs, head_step, 0)
        if between is not None:
            between()
        if q > 0:
            z_copy(q - 1).wait()

        def out_step(step, carry):
            index = step + pairs
            buf = lax.rem(index, DEEP)
            ahead = lax.rem(index + DEEP - 1, DEEP)

            @pl.when(step + DEEP - 1 < outs)
            def _():
                start_all(out_copies(step + DEEP - 1, ahead))

            if q + 1 < chunks:
                @pl.when(step + DEEP - 1 >= outs)
                def _():
                    start_all(qkv_copies(step + DEEP - 1 - outs, ahead))

            for copy in out_copies(step, buf):
                copy.wait()
            for i in range(2):
                lanes = pl.ds(pl.multiple_of(step * 2 * COLS + i * COLS, COLS), COLS)
                proj = jnp.dot(ctx[:size], wtile[buf, i], preferred_element_type=F32).astype(BF16).astype(F32)
                zbuf[:size, lanes] = (yrecv[pl.ds(start, size), lanes].astype(F32) + proj).astype(BF16)
            return carry

        lax.fori_loop(0, outs, out_step, 0)
        z_copy(q).start()

    residual(0).start()
    partials(0)
    pass_on(0)
    own_partials(0)
    partials(1)
    finish(0)
    for q in range(1, chunks):
        if q + 1 < chunks:
            partials(q + 1)
        pass_on(q)
        own_partials(q)
        if q < chunks - 1:
            attend(q - 1)
            finish(q)
        else:
            attend(q - 1, functools.partial(finish, q))
    attend(chunks - 1)

    z_copy(chunks - 1).wait()
    for copy in meta_copies:
        copy.wait_send()
    for slot, side in first_blocks + own_blocks:
        partner_rows(slot, side).wait_send()
    for q in range(chunks):
        y_copy(q).wait_send()
        for way in (0, 1):
            if q >= chunks - 2:
                ring_copy(q, 1, way).wait_send()
                ring_copy(q, 2, way).wait_send()


def fused_call(meta, gain, expert_out, resid, w_query, w_key, w_value, w_out, head_dim, ring, stages):
    experts, capacity, width = expert_out.shape
    seq_len = resid.shape[0]
    slot_dev = capacity // (ring * CORES)
    half = width // 2
    depth = CORES * experts * slot_dev
    chunks = len(SIZES)
    largest = max(SIZES)
    assert sum(SIZES) == seq_len and w_query.shape[1] == width
    dims = (ring, stages, experts, slot_dev, width, seq_len, 6, head_dim)
    dma = pltpu.SemaphoreType.DMA
    anywhere = pl.BlockSpec(memory_space=pl.ANY)
    local = pl.BlockSpec(memory_space=pltpu.VMEM)
    return pl.pallas_call(
        functools.partial(fused_kernel, dims),
        out_shape=[jax.ShapeDtypeStruct((seq_len, width), BF16),
                   jax.ShapeDtypeStruct((4, 2, experts, slot_dev, half), BF16)],
        in_specs=[local, local] + [anywhere] * 6,
        out_specs=[anywhere, anywhere],
        scratch_shapes=[
            pltpu.VMEM((2, CORES, experts, slot_dev, half), BF16),
            pltpu.VMEM((3, 16, seq_len), F32),
            pltpu.VMEM((seq_len, 16), F32),
            pltpu.VMEM((2, 3 * largest, depth), BF16),
            pltpu.VMEM((2, 3, 2, largest, half), F32),
            pltpu.VMEM((3, 2, seq_len, half), F32),
            pltpu.VMEM((seq_len, width), BF16),
            pltpu.VMEM((seq_len, width), BF16),
            pltpu.VMEM((largest, width), BF16),
            pltpu.VMEM((DEEP, 3, width, COLS), BF16),
            pltpu.VMEM((seq_len, width), BF16),
            pltpu.VMEM((seq_len, width), BF16),
            pltpu.VMEM((largest, width), BF16),
            pltpu.VMEM((largest, width), BF16),
            pltpu.VMEM((largest, width), BF16),
            dma((2, 2)), dma((4, 2)), dma((4, 2)),
            dma((3,)), dma((3,)),
            dma((chunks, 3, 2)), dma((chunks, 3, 2)),
            dma((chunks,)), dma((chunks,)),
            dma, dma((DEEP, 3)), dma,
        ],
        compiler_params=pltpu.CompilerParams(collective_id=0, has_side_effects=True, vmem_limit_bytes=67_043_328),
        name='combine_attend',
    )(meta, gain, expert_out, resid, w_query, w_key, w_value, w_out)[0]


def solution(mesh):
    stages = mesh.shape['pp']
    ep_size = mesh.shape['ep']
    ring = ep_size // CORES
    assert ring == 4
    token_spec = P(('data', 'pp'), None, 'ep', None, None)
    weight_spec = P('pp', None, None)

    def local_step(expert_out, expert_ids, slot_ids, gates, resid, norm_scale, w_query, w_key, w_value, w_out):
        experts, capacity, width = expert_out.shape[2:]
        slot_dev = capacity // ep_size
        ids, slots, gate = expert_ids[0, 0, 0], slot_ids[0, 0, 0], gates[0, 0, 0]
        keys = jnp.where(slots >= 0, ids * slot_dev + slots - lax.axis_index('ep') * slot_dev, -1).astype(F32)
        pad = ((0, 8 - keys.shape[1]), (0, 0))
        meta = jnp.concatenate([jnp.pad(keys.T, pad), jnp.pad(gate.T, pad)], axis=0)
        heads, head_dim = w_out.shape[1:3]
        z = fused_call(meta, norm_scale, expert_out[0, 0], resid[0, 0, 0], w_query[0], w_key[0], w_value[0],
                       w_out[0].reshape(heads * head_dim, width), head_dim, ring, stages)
        return z[None, None, None]

    return jax.shard_map(local_step, mesh=mesh, in_specs=(token_spec, token_spec, token_spec, token_spec, token_spec, P('pp', None), weight_spec, weight_spec, weight_spec, P('pp', None, None, None)), out_specs=token_spec, check_vma=False)
```

```python
import functools

import jax
import jax.numpy as jnp
from jax import lax
from jax.experimental import pallas as pl
from jax.experimental.pallas import tpu as pltpu
from jax.sharding import PartitionSpec as P

NORM_EPS = 1e-6
CORES = 2
SIZES = (160, 144, 128, 80)
HOOK = 4
MESH = pl.DeviceIdType.MESH
F32 = jnp.float32
BF16 = jnp.bfloat16
LANES = 128
COLS = 256
DEEP = 3


def fused_kernel(dims, meta_ref, gain_ref, eo_ref, h_ref, wq_ref, wk_ref, wv_ref, wo_ref, z_ref, prow,
                 obuf, metas, mt, wbuf, part, recv, ybuf, yrecv, hbuf, wtile, kc, vc, xs, ctx, zbuf,
                 b_sem, o_send, o_recv, m_send, m_recv, r_send, r_recv, y_send, y_recv, h_sem, w_sem, z_sem):
    ring, stages, experts, slot_dev, width, seq_len, top_k, head_dim = dims
    half = width // 2
    depth = CORES * experts * slot_dev
    starts = [sum(SIZES[:q]) for q in range(len(SIZES))]
    chunks = len(SIZES)
    ep = lax.axis_index('ep')
    stage = lax.axis_index('pp')
    chip = ep // CORES
    core = ep % CORES
    other = 1 - core

    def chip_at(offset):
        return lax.rem(chip + offset + ring, ring)

    def ep_at(offset):
        return {'ep': chip_at(offset) * CORES + core}

    partner = {'ep': chip * CORES + other}
    next_stage = {'pp': lax.rem(stage + 1, stages)}
    prev_stage = {'pp': lax.rem(stage + stages - 1, stages)}
    offsets = (-1, 1, 2, 0)

    barrier = pltpu.get_barrier_semaphore()
    peers = (partner, ep_at(-1), ep_at(1), ep_at(2), next_stage, prev_stage)
    for peer in peers:
        pl.semaphore_signal(barrier, inc=1, device_id=peer, device_id_type=MESH)
    pl.semaphore_wait(barrier, len(peers))

    def partner_rows(slot, side):
        rows = pl.ds((chip_at(offsets[slot]) * CORES + other) * slot_dev, slot_dev)
        return pltpu.make_async_remote_copy(
            src_ref=eo_ref.at[:, rows, pl.ds(side * half, half)], dst_ref=prow.at[slot, side],
            send_sem=o_send.at[slot, side], recv_sem=o_recv.at[slot, side], device_id=partner, device_id_type=MESH)

    meta_copies = [pltpu.make_async_remote_copy(
        src_ref=meta_ref, dst_ref=metas.at[slot], send_sem=m_send.at[slot], recv_sem=m_recv.at[slot],
        device_id=ep_at(-offsets[slot]), device_id_type=MESH) for slot in range(3)]
    first_blocks = ((2, 0), (2, 1), (1, 1), (0, 0), (1, 0), (0, 1))
    own_blocks = ((3, 0), (3, 1))
    for copy in meta_copies:
        copy.start()
    for slot, side in first_blocks + own_blocks:
        partner_rows(slot, side).start()

    uses = list(first_blocks) + list(own_blocks) + list(first_blocks) * 2 + list(own_blocks) + list(first_blocks) \
        + list(own_blocks) * 2
    arrived = set()

    def block_copies(index):
        slot, side = uses[index]
        buf = index % 2
        rows = pl.ds((chip_at(offsets[slot]) * CORES + core) * slot_dev, slot_dev)
        mine = pltpu.make_async_copy(eo_ref.at[:, rows, pl.ds(side * half, half)], obuf.at[buf, core], b_sem.at[buf, 0])
        theirs = pltpu.make_async_copy(prow.at[slot, side], obuf.at[buf, other], b_sem.at[buf, 1])
        return mine, theirs

    def fetch_block(index):
        if index < len(uses):
            mine, theirs = block_copies(index)
            mine.start()
            if uses[index] not in arrived:
                arrived.add(uses[index])
                partner_rows(*uses[index]).wait_recv()
            theirs.start()

    pairs = width // COLS
    outs = pairs // 2
    steps = pairs + outs

    def qkv_copies(step, buf):
        cols = pl.ds(pl.multiple_of(step * COLS, COLS), COLS)
        return [pltpu.make_async_copy(ref.at[:, cols], wtile.at[buf, i], w_sem.at[buf, i])
                for i, ref in enumerate((wq_ref, wk_ref, wv_ref))]

    def out_copies(step, buf):
        return [pltpu.make_async_copy(wo_ref.at[:, pl.ds(pl.multiple_of(step * 2 * COLS + i * COLS, COLS), COLS)],
                                      wtile.at[buf, i], w_sem.at[buf, i]) for i in range(2)]

    def start_all(copies):
        for copy in copies:
            copy.start()

    fetch_block(0)
    for step in range(DEEP - 1):
        start_all(qkv_copies(step, step))

    def zero_step(i, carry):
        at = pl.ds(pl.multiple_of(i * 16, 16), 16)
        kc[at, :] = jnp.zeros((16, width), BF16)
        vc[at, :] = jnp.zeros((16, width), BF16)
        return carry

    lax.fori_loop(0, seq_len // 16, zero_step, 0)

    base = (chip * depth).astype(F32)
    lane = lax.broadcasted_iota(jnp.int32, (16, LANES), 1).astype(F32) + base
    met = set()

    def build(bank, slot, q):
        if slot < 3 and slot not in met:
            met.add(slot)
            meta_copies[slot].wait_recv()
        size = SIZES[q]
        for lo in range(0, seq_len, LANES):
            if lo < starts[q] + size and lo + LANES > starts[q]:
                cols = slice(lo, lo + LANES)
                block = meta_ref[:, cols] if slot == 3 else metas[slot, :, cols]
                mt[lo:lo + LANES, :] = jnp.transpose(block)

        def rows_step(step, carry):
            at = pl.multiple_of(step * 16, 16)
            rows = mt[pl.ds(starts[q] + at, 16), :]
            keys = [jnp.broadcast_to(rows[:, k:k + 1], (16, LANES)) for k in range(top_k)]
            gates = [jnp.broadcast_to(rows[:, 8 + k:9 + k], (16, LANES)) for k in range(top_k)]
            for tile in range(depth // LANES):
                place = lane + float(tile * LANES)
                weight = jnp.zeros((16, LANES), F32)
                for k in range(top_k):
                    weight = jnp.where(keys[k] == place, gates[k], weight)
                high = weight.astype(BF16)
                rest = weight - high.astype(F32)
                mid = rest.astype(BF16)
                low = (rest - mid.astype(F32)).astype(BF16)
                at_col = slice(tile * LANES, (tile + 1) * LANES)
                wbuf[bank, pl.ds(at, 16), at_col] = high
                wbuf[bank, pl.ds(size + at, 16), at_col] = mid
                wbuf[bank, pl.ds(2 * size + at, 16), at_col] = low
            return carry

        lax.fori_loop(0, size // 16, rows_step, 0)

    used = [0]

    def weigh(bank, slot, side, q, dst):
        index = used[0]
        used[0] += 1
        assert uses[index] == (slot, side)
        size = SIZES[q]
        buf = index % 2
        fetch_block(index + 1)
        for copy in block_copies(index):
            copy.wait()

        def step(tile, carry):
            at = pl.multiple_of(tile * COLS, COLS)
            rows = obuf[buf, :, :, :, pl.ds(at, COLS)].reshape(depth, COLS)
            res = jnp.dot(wbuf[bank, :3 * size], rows, preferred_element_type=F32)
            dst[:size, pl.ds(at, COLS)] = (res[2 * size:] + res[size:2 * size]) + res[:size]
            return carry

        lax.fori_loop(0, half // COLS, step, 0)

    sent = (((2, 0), (2, 1)), ((1, 1), (0, 0)), ((1, 0), (0, 1)))

    def ring_copy(q, kind, way):
        slot, side = sent[kind][way]
        rows = pl.ds(starts[q], SIZES[q])
        return pltpu.make_async_remote_copy(
            src_ref=part.at[q % 2, slot, side, pl.ds(0, SIZES[q])], dst_ref=recv.at[kind, way, rows],
            send_sem=r_send.at[q, kind, way], recv_sem=r_recv.at[q, kind, way],
            device_id=ep_at(1 if way == 0 else -1), device_id_type=MESH)

    def residual(q):
        return pltpu.make_async_copy(h_ref.at[pl.ds(starts[q], SIZES[q])], hbuf.at[pl.ds(0, SIZES[q])], h_sem)

    def partials(q, send):
        par = part.at[q % 2]
        if q >= 2:
            for way in (0, 1):
                ring_copy(q - 2, 1, way).wait_send()
                ring_copy(q - 2, 2, way).wait_send()
        build(0, 2, q)
        weigh(0, 2, 0, q, par.at[2, 0])
        if send:
            ring_copy(q, 0, 0).start()
        weigh(0, 2, 1, q, par.at[2, 1])
        if send:
            ring_copy(q, 0, 1).start()
        build(1, 1, q)
        weigh(1, 1, 1, q, par.at[1, 1])
        if send:
            ring_copy(q, 1, 0).start()
        build(0, 0, q)
        weigh(0, 0, 0, q, par.at[0, 0])
        if send:
            ring_copy(q, 1, 1).start()
        weigh(1, 1, 0, q, par.at[1, 0])
        weigh(0, 0, 1, q, par.at[0, 1])

    def send_partials(q):
        for kind in (0, 1):
            for way in (0, 1):
                ring_copy(q, kind, way).start()

    def pass_on(q):
        for way in (0, 1):
            slot, side = sent[2][way]
            ring_copy(q, 0, way).wait_recv()

            def rows_step(i, carry, way=way, slot=slot, side=side):
                at = pl.multiple_of(i * 16, 16)
                mine = part[q % 2, slot, side, pl.ds(at, 16), :]
                part[q % 2, slot, side, pl.ds(at, 16), :] = mine + recv[0, way, pl.ds(starts[q] + at, 16), :]
                return carry

            lax.fori_loop(0, SIZES[q] // 16, rows_step, 0)
            ring_copy(q, 2, way).start()

    def own_partials(q):
        for way in (0, 1):
            ring_copy(q, 0, way).wait_send()
        build(0, 3, q)
        for side in (0, 1):
            weigh(0, 3, side, q, part.at[q % 2, 2, side])

    def y_copy(q):
        return pltpu.make_async_remote_copy(
            src_ref=ybuf.at[pl.ds(starts[q], SIZES[q])], dst_ref=yrecv.at[pl.ds(starts[q], SIZES[q])],
            send_sem=y_send.at[q], recv_sem=y_recv.at[q], device_id=next_stage, device_id_type=MESH)

    def finish(q):
        residual(q).wait()
        for way in (0, 1):
            ring_copy(q, 1, way).wait_recv()
            ring_copy(q, 2, way).wait_recv()
        for side in (0, 1):

            def rows_step(i, carry, side=side):
                at = pl.multiple_of(i * 16, 16)
                rows = pl.ds(starts[q] + at, 16)
                cols = slice(side * half, (side + 1) * half)
                total = part[q % 2, 2, side, pl.ds(at, 16), :]
                total = total + recv[1, 1 - side, rows, :]
                total = total + recv[2, side, rows, :]
                total = total + hbuf[pl.ds(at, 16), cols].astype(F32)
                ybuf[rows, cols] = total.astype(BF16)
                return carry

            lax.fori_loop(0, SIZES[q] // 16, rows_step, 0)
        y_copy(q).start()
        if q + 1 < chunks:
            residual(q + 1).start()

    def z_copy(q):
        return pltpu.make_async_copy(zbuf.at[pl.ds(0, SIZES[q])], z_ref.at[pl.ds(starts[q], SIZES[q])], z_sem)

    def attend(q, between=None):
        size, start = SIZES[q], starts[q]
        seen = -(-(start + size) // LANES) * LANES
        y_copy(q).wait_recv()

        def norm_step(i, carry):
            at = pl.multiple_of(i * 16, 16)
            x = yrecv[pl.ds(start + at, 16), :].astype(F32)
            inv_rms = lax.rsqrt(jnp.mean(x * x, axis=-1, keepdims=True) + NORM_EPS)
            xs[pl.ds(at, 16), :] = (x * inv_rms * gain_ref[...]).astype(BF16)
            return carry

        lax.fori_loop(0, size // 16, norm_step, 0)
        row = lax.broadcasted_iota(jnp.int32, (size, seen), 0) + start
        col = lax.broadcasted_iota(jnp.int32, (size, seen), 1)

        def head_step(step, carry):
            buf = lax.rem(step, DEEP)
            ahead = lax.rem(step + DEEP - 1, DEEP)

            @pl.when(step + DEEP - 1 < pairs)
            def _():
                start_all(qkv_copies(step + DEEP - 1, ahead))

            @pl.when(step + DEEP - 1 >= pairs)
            def _():
                start_all(out_copies(step + DEEP - 1 - pairs, ahead))

            for copy in qkv_copies(step, buf):
                copy.wait()
            x = xs[:size]
            lanes = pl.ds(pl.multiple_of(step * COLS, COLS), COLS)
            qh = jnp.dot(x, wtile[buf, 0], preferred_element_type=F32).astype(BF16)
            kc[pl.ds(start, size), lanes] = jnp.dot(x, wtile[buf, 1], preferred_element_type=F32).astype(BF16)
            vc[pl.ds(start, size), lanes] = jnp.dot(x, wtile[buf, 2], preferred_element_type=F32).astype(BF16)
            for head in range(COLS // head_dim):
                one = pl.ds(pl.multiple_of(step * COLS + head * head_dim, head_dim), head_dim)
                s = lax.dot_general(qh[:, head * head_dim:(head + 1) * head_dim], kc[:seen, one],
                                    (((1,), (1,)), ((), ())), preferred_element_type=F32) * head_dim ** -0.5
                s = jnp.where(row >= col, s, -jnp.inf)
                e = jnp.exp(s - jnp.max(s, axis=-1, keepdims=True))
                p = (e * (1.0 / jnp.sum(e, axis=-1, keepdims=True))).astype(BF16)
                ctx[:size, one] = jnp.dot(p, vc[:seen, one], preferred_element_type=F32).astype(BF16)
            return carry

        if between is None:
            lax.fori_loop(0, pairs, head_step, 0)
        else:
            lax.fori_loop(0, HOOK, head_step, 0)
            between()
            lax.fori_loop(HOOK, pairs, head_step, 0)
        if q > 0:
            z_copy(q - 1).wait()

        def out_step(step, carry):
            index = step + pairs
            buf = lax.rem(index, DEEP)
            ahead = lax.rem(index + DEEP - 1, DEEP)

            @pl.when(step + DEEP - 1 < outs)
            def _():
                start_all(out_copies(step + DEEP - 1, ahead))

            if q + 1 < chunks:
                @pl.when(step + DEEP - 1 >= outs)
                def _():
                    start_all(qkv_copies(step + DEEP - 1 - outs, ahead))

            for copy in out_copies(step, buf):
                copy.wait()
            for i in range(2):
                lanes = pl.ds(pl.multiple_of(step * 2 * COLS + i * COLS, COLS), COLS)
                proj = jnp.dot(ctx[:size], wtile[buf, i], preferred_element_type=F32).astype(BF16).astype(F32)
                zbuf[:size, lanes] = (yrecv[pl.ds(start, size), lanes].astype(F32) + proj).astype(BF16)
            return carry

        lax.fori_loop(0, outs, out_step, 0)
        z_copy(q).start()

    residual(0).start()
    partials(0, True)
    pass_on(0)
    own_partials(0)
    partials(1, True)
    finish(0)
    for q in range(1, chunks):
        if q + 1 < chunks:
            partials(q + 1, False)
        pass_on(q)
        if q + 1 < chunks:
            send_partials(q + 1)
        own_partials(q)
        if q < chunks - 1:
            attend(q - 1)
            finish(q)
        else:
            attend(q - 1, functools.partial(finish, q))
    attend(chunks - 1)

    z_copy(chunks - 1).wait()
    for copy in meta_copies:
        copy.wait_send()
    for slot, side in first_blocks + own_blocks:
        partner_rows(slot, side).wait_send()
    for q in range(chunks):
        y_copy(q).wait_send()
        for way in (0, 1):
            if q >= chunks - 2:
                ring_copy(q, 1, way).wait_send()
                ring_copy(q, 2, way).wait_send()


def fused_call(meta, gain, expert_out, resid, w_query, w_key, w_value, w_out, head_dim, ring, stages):
    experts, capacity, width = expert_out.shape
    seq_len = resid.shape[0]
    slot_dev = capacity // (ring * CORES)
    half = width // 2
    depth = CORES * experts * slot_dev
    chunks = len(SIZES)
    largest = max(SIZES)
    assert sum(SIZES) == seq_len and w_query.shape[1] == width
    dims = (ring, stages, experts, slot_dev, width, seq_len, 6, head_dim)
    dma = pltpu.SemaphoreType.DMA
    anywhere = pl.BlockSpec(memory_space=pl.ANY)
    local = pl.BlockSpec(memory_space=pltpu.VMEM)
    return pl.pallas_call(
        functools.partial(fused_kernel, dims),
        out_shape=[jax.ShapeDtypeStruct((seq_len, width), BF16),
                   jax.ShapeDtypeStruct((4, 2, experts, slot_dev, half), BF16)],
        in_specs=[local, local] + [anywhere] * 6,
        out_specs=[anywhere, anywhere],
        scratch_shapes=[
            pltpu.VMEM((2, CORES, experts, slot_dev, half), BF16),
            pltpu.VMEM((3, 16, seq_len), F32),
            pltpu.VMEM((seq_len, 16), F32),
            pltpu.VMEM((2, 3 * largest, depth), BF16),
            pltpu.VMEM((2, 3, 2, largest, half), F32),
            pltpu.VMEM((3, 2, seq_len, half), F32),
            pltpu.VMEM((seq_len, width), BF16),
            pltpu.VMEM((seq_len, width), BF16),
            pltpu.VMEM((largest, width), BF16),
            pltpu.VMEM((DEEP, 3, width, COLS), BF16),
            pltpu.VMEM((seq_len, width), BF16),
            pltpu.VMEM((seq_len, width), BF16),
            pltpu.VMEM((largest, width), BF16),
            pltpu.VMEM((largest, width), BF16),
            pltpu.VMEM((largest, width), BF16),
            dma((2, 2)), dma((4, 2)), dma((4, 2)),
            dma((3,)), dma((3,)),
            dma((chunks, 3, 2)), dma((chunks, 3, 2)),
            dma((chunks,)), dma((chunks,)),
            dma, dma((DEEP, 3)), dma,
        ],
        compiler_params=pltpu.CompilerParams(collective_id=0, has_side_effects=True, vmem_limit_bytes=67_043_328),
        name='combine_attend',
    )(meta, gain, expert_out, resid, w_query, w_key, w_value, w_out)[0]


def solution(mesh):
    stages = mesh.shape['pp']
    ep_size = mesh.shape['ep']
    ring = ep_size // CORES
    assert ring == 4
    token_spec = P(('data', 'pp'), None, 'ep', None, None)
    weight_spec = P('pp', None, None)

    def local_step(expert_out, expert_ids, slot_ids, gates, resid, norm_scale, w_query, w_key, w_value, w_out):
        experts, capacity, width = expert_out.shape[2:]
        slot_dev = capacity // ep_size
        ids, slots, gate = expert_ids[0, 0, 0], slot_ids[0, 0, 0], gates[0, 0, 0]
        keys = jnp.where(slots >= 0, ids * slot_dev + slots - lax.axis_index('ep') * slot_dev, -1).astype(F32)
        pad = ((0, 8 - keys.shape[1]), (0, 0))
        meta = jnp.concatenate([jnp.pad(keys.T, pad), jnp.pad(gate.T, pad)], axis=0)
        heads, head_dim = w_out.shape[1:3]
        z = fused_call(meta, norm_scale, expert_out[0, 0], resid[0, 0, 0], w_query[0], w_key[0], w_value[0],
                       w_out[0].reshape(heads * head_dim, width), head_dim, ring, stages)
        return z[None, None, None]

    return jax.shard_map(local_step, mesh=mesh, in_specs=(token_spec, token_spec, token_spec, token_spec, token_spec, P('pp', None), weight_spec, weight_spec, weight_spec, P('pp', None, None, None)), out_specs=token_spec, check_vma=False)
```
